256 devices in a mesh: rep: 16 (over x_hi, z), atom: 16 (over x_lo, y, core).
Axes of the slice: x: 4 (x_hi: 2, x_lo: 2; x = x_hi * 2 + x_lo), y: 4, z: 8, core: 2. Of those that a mesh axis runs over, the one named last changes fastest.
Arguments:
- starting_locations: float32 [64, 3, 16384], P('rep', None, 'atom'), may hold values from 0 to 16
- starting_speeds: float32 [64, 3, 16384], P('rep', None, 'atom'), may hold values from -5 to 5
- terminal_location_adjoint: float32 [64, 3, 16384], P('rep', None, 'atom'), may hold values from -6 to 6
- terminal_speed_adjoint: float32 [64, 3, 16384], P('rep', None, 'atom'), may hold values from -7.5 to 7.5
- interaction_strength: float32 [16384], P('atom'), may hold values from 0.5 to 2
- reciprocal_particle_weight: float32 [16384], P('atom'), may hold values from 0.05 to 2
- heat_levels: float32 [64], P('rep'), may hold values from 0.25 to 4
- swap_indicator: int32 [64], P('rep'), may hold values from 0 to 1, as said below
- companion_group_indices: int32 [5, 128, 2], P(None, 'atom'), may hold values from 0 to 23, as said below
Outputs:
- final_pos: float32 [64, 3, 16384], P('rep', None, 'atom')
- final_vel: float32 [64, 3, 16384], P('rep', None, 'atom')
- energies: float32 [64], P('rep')
- grad_pos: float32 [64, 3, 16384], P('rep', None, 'atom')
- grad_vel: float32 [64, 3, 16384], P('rep', None, 'atom')
- grad_coupling: float32 [16384], P('atom')
The draws below stay inside these ranges and needn't reach their ends.
Inputs may be any that keep to these rules, and one draw needn't show every extreme that they name: `swap_indicator`: replicas r and r + 4, for r with r // 4 even, carry the same flag; among the replicas r to r + 3, for r a multiple of 8, at least one carries 1. `companion_group_indices`: the 2 entries of a row differ.
All inputs are finite; a program needn't handle non-finite values.
Results may differ from the reference program's by a relative error of at most 0.0003.
Values sent between devices are 32-bit elements; how exact they have to be, the bound alone decides.
No kernel may reach another device: no remote copies, remote signals or barrier semaphores. Data moves between devices by JAX's collectives and lax.ppermute only.
A program may use at most 64 MiB of HBM per device.

```python
import math
import jax
import jax.numpy as jnp
from jax import lax

BLOCK = 128
BLOCKS_DEV = 8
PARTNERS = 2
STEPS = 4
REP_DEV = 4
ATOMS = 16384
WALKER_TOTAL = 64


def draw_starting_locations(key, part):
    grid_shape = (WALKER_TOTAL, ATOMS)
    subkeys = jax.random.split(key, 3)
    inside = jax.random.uniform(subkeys[0], grid_shape)
    owner = (jnp.arange(ATOMS, dtype=jnp.int32) // (BLOCKS_DEV * BLOCK)).astype(jnp.float32)
    along_axis = owner[None, :] + inside
    cross_side = 2.0
    side_axis = jax.random.uniform(subkeys[1], grid_shape) * cross_side
    depth_axis = jax.random.uniform(subkeys[2], grid_shape) * cross_side
    return jnp.stack([along_axis, side_axis, depth_axis], axis=1).astype(jnp.float32)


def motion_noise(key):
    base_key = jax.random.fold_in(key, 101)
    return jnp.clip(jax.random.normal(base_key, (WALKER_TOTAL, 3, ATOMS)), -5.0, 5.0)


def draw_starting_speeds(key, part):
    return motion_noise(key).astype(jnp.float32)


def draw_terminal_speed_adjoint(key, part):
    fresh_noise = jnp.clip(jax.random.normal(jax.random.fold_in(key, 202), (WALKER_TOTAL, 3, ATOMS)), -5.0, 5.0)
    return (0.5 * motion_noise(key) + fresh_noise).astype(jnp.float32)


def draw_reciprocal_particle_weight(key, part):
    ramp_up = jnp.arange(ATOMS, dtype=jnp.float32) / ATOMS
    roughness = jnp.exp(jax.random.uniform(key, (ATOMS,), minval=jnp.log(0.5), maxval=jnp.log(2.0)))
    return (roughness / (1.0 + 2.0 * ramp_up)).astype(jnp.float32)


def draw_swap_indicator(key, part):
    groups = WALKER_TOTAL // (2 * REP_DEV)
    flag_key = jax.random.fold_in(key, 303)
    slot_key = jax.random.fold_in(key, 404)
    base_flags = jax.random.randint(flag_key, (groups, REP_DEV), 0, 2)
    forced_slot = jax.random.randint(slot_key, (groups, 1), 0, REP_DEV)
    forced = (jnp.arange(REP_DEV, dtype=jnp.int32)[None, :] == forced_slot).astype(jnp.int32)
    base_flags = jnp.maximum(base_flags, forced)
    spread = jnp.broadcast_to(base_flags[:, None, :], (groups, 2, REP_DEV))
    return spread.reshape(WALKER_TOTAL).astype(jnp.int32)


def draw_companion_group_indices(key, part):
    slot_count = 3 * BLOCKS_DEV
    scores = jax.random.randint(key, (STEPS + 1, ATOMS // BLOCK, slot_count), 0, 1 << 20)
    scores = scores * slot_count + jnp.arange(slot_count, dtype=jnp.int32)
    return lax.top_k(scores, PARTNERS)[1].astype(jnp.int32)


def level_of(own_key, dims, cuts, smallest, top_value):
    def one(axis_at, blocks):
        heights = jax.random.uniform(jax.random.fold_in(jax.random.fold_in(own_key, 6), axis_at), (blocks,), jnp.float32, smallest / len(cuts), top_value / len(cuts))
        return jnp.repeat(jnp.exp(heights), dims[axis_at] // blocks).reshape((-1,) + (1,) * (len(dims) - axis_at - 1))

    factor_of = one(*cuts[0])
    for cut in cuts[1:]:
        factor_of = factor_of * one(*cut)
    return factor_of


def noise(stream_key, dims, deviation, limit, pieces=(), kind=jnp.bfloat16):
    drawn = deviation * jax.random.normal(stream_key, dims, jnp.float32)
    if pieces:
        drawn = drawn * level_of(stream_key, dims, pieces, -0.22, 0.18)
    return jnp.clip(drawn, -limit, limit).astype(kind)


def setup_inputs(seed: int = 0) -> dict:
    arg_keys = jax.random.split(jax.random.key(seed), 10)
    return {
        "starting_locations": draw_starting_locations(jax.random.fold_in(arg_keys[9], 71), 0),
        "starting_speeds": draw_starting_speeds(jax.random.fold_in(arg_keys[9], 71), 0),
        "terminal_location_adjoint": noise(arg_keys[2], (WALKER_TOTAL, 3, ATOMS), 1.0, 6.0, ((0, 16), (2, 16)), jnp.float32),
        "terminal_speed_adjoint": draw_terminal_speed_adjoint(jax.random.fold_in(arg_keys[9], 71), 0),
        "interaction_strength": jnp.clip(jnp.exp(math.log(2.0) - 1.3862944 * jax.random.uniform(arg_keys[4], (ATOMS,), jnp.float32) ** level_of(arg_keys[4], (ATOMS,), ((0, 16),), -0.2, 0.2)), 0.5, 2.0),
        "reciprocal_particle_weight": draw_reciprocal_particle_weight(jax.random.fold_in(arg_keys[9], 71), 0),
        "heat_levels": jnp.clip(jnp.exp(math.log(4.0) - 2.7725887 * jax.random.uniform(arg_keys[6], (WALKER_TOTAL,), jnp.float32) ** level_of(arg_keys[6], (WALKER_TOTAL,), ((0, 16),), -0.2, 0.2)), 0.25, 4.0),
        "swap_indicator": draw_swap_indicator(jax.random.fold_in(arg_keys[9], 71), 0),
        "companion_group_indices": draw_companion_group_indices(jax.random.fold_in(arg_keys[9], 71), 0),
    }


TIME_STEP = 0.05
THERMO_RELAX = 0.5
KINETIC_EPSILON = 1e-06

def walker_energy(particle_location, interaction_strength, lists_now):
    padding = BLOCKS_DEV * BLOCK
    block_total = ATOMS // BLOCK
    padded_pos = jnp.pad(particle_location, ((0, 0), (padding, padding))).reshape(3, block_total + 2 * BLOCKS_DEV, BLOCK)
    padded_coupling = jnp.pad(interaction_strength, (padding, padding)).reshape(block_total + 2 * BLOCKS_DEV, BLOCK)
    block_ids = jnp.arange(block_total, dtype=jnp.int32)
    chosen = (block_ids // BLOCKS_DEV * BLOCKS_DEV)[:, None] + lists_now
    own_block = particle_location.reshape(3, block_total, BLOCK)
    far_block = padded_pos[:, chosen]
    squared = jnp.zeros((block_total, PARTNERS, BLOCK, BLOCK), particle_location.dtype)
    for axis_id in range(3):
        offset = own_block[axis_id][:, None, :, None] - far_block[axis_id][:, :, None, :]
        squared = squared + offset * offset
    self_block = lists_now == (BLOCKS_DEV + block_ids % BLOCKS_DEV)[:, None]
    diagonal = jnp.arange(BLOCK)[:, None] == jnp.arange(BLOCK)[None, :]
    kept_pairs = 1.0 - (self_block[:, :, None, None] & diagonal).astype(particle_location.dtype)
    weight = interaction_strength.reshape(block_total, BLOCK)[:, None, :, None] * padded_coupling[chosen][:, :, None, :]
    strength = BLOCKS_DEV / (8.0 * PARTNERS)
    return 0.5 * strength * jnp.sum(weight * jnp.exp(-0.5 * squared) * kept_pairs)

def force_and_energy(particle_location, interaction_strength, lists_now):
    energy, gradient = jax.value_and_grad(walker_energy)(particle_location, interaction_strength, lists_now)
    return (-gradient, energy)

def trajectory(opening_location, opening_speed, interaction_strength, reciprocal_particle_weight, companion_group_indices, leading_heat_level, trailing_heat_level):
    stepper = jax.checkpoint(force_and_energy)
    half_step = 0.5 * TIME_STEP
    push_vectors, energy = stepper(opening_location, interaction_strength, companion_group_indices[0])
    particle_location, particle_speed, desired_heat_level = (opening_location, opening_speed, leading_heat_level)
    for iteration_number in range(STEPS):
        if iteration_number == STEPS // 2:
            particle_speed = particle_speed * jnp.sqrt(trailing_heat_level / leading_heat_level)
            desired_heat_level = trailing_heat_level
        mid_velocity = particle_speed + half_step * reciprocal_particle_weight * push_vectors
        particle_location = particle_location + TIME_STEP * mid_velocity
        push_vectors, energy = stepper(particle_location, interaction_strength, companion_group_indices[iteration_number + 1])
        updated = mid_velocity + half_step * reciprocal_particle_weight * push_vectors
        kinetic = 0.5 * jnp.sum(updated * updated / reciprocal_particle_weight)
        present_state = 2.0 * kinetic / (3 * ATOMS) + KINETIC_EPSILON
        rescaling_multiplier = jnp.sqrt(1.0 + THERMO_RELAX * (desired_heat_level / present_state - 1.0))
        particle_speed = rescaling_multiplier * updated
    return ((particle_location, particle_speed), energy / ATOMS)

def reference(starting_locations, starting_speeds, terminal_location_adjoint, terminal_speed_adjoint, interaction_strength, reciprocal_particle_weight, heat_levels, swap_indicator, companion_group_indices):
    walker_ids = jnp.arange(WALKER_TOTAL, dtype=jnp.int32)
    swap_companion = jnp.where(walker_ids // REP_DEV % 2 == 0, walker_ids + REP_DEV, walker_ids - REP_DEV)
    upcoming_heat_level = jnp.where(swap_indicator == 1, heat_levels[swap_companion], heat_levels)

    def lone_walker(collapsed_total, sliced):
        walker_pos, walker_vel, leading_heat_level, trailing_heat_level, walker_cot_pos, walker_cot_vel = sliced

        def rollout(particle_location, particle_speed, couplings):
            return trajectory(particle_location, particle_speed, couplings, reciprocal_particle_weight, companion_group_indices, leading_heat_level, trailing_heat_level)
        finals, pullback, energy = jax.vjp(rollout, walker_pos, walker_vel, interaction_strength, has_aux=True)
        grad_position, grad_velocity, grad_couplings = pullback((walker_cot_pos, walker_cot_vel))
        return (collapsed_total + grad_couplings, (finals[0], finals[1], energy, grad_position, grad_velocity))
    collapsed_total, gathered_results = lax.scan(lone_walker, jnp.zeros_like(interaction_strength), (starting_locations, starting_speeds, heat_levels, upcoming_heat_level, terminal_location_adjoint, terminal_speed_adjoint))
    return (gathered_results[0], gathered_results[1], gathered_results[2], gathered_results[3], gathered_results[4], collapsed_total)
```

```python
import jax
import jax.numpy as jnp
from jax import lax
from jax.experimental import pallas as pl
from jax.experimental.pallas import tpu as pltpu
from jax.sharding import PartitionSpec as P

TIME_STEP = 0.05
THERMO_RELAX = 0.5
KINETIC_EPSILON = 1e-06
LOG2E = 1.4426950408889634
FAR = -1.0e5

F32 = jnp.float32
BF16 = jnp.bfloat16

LANES = 128
EDGE = 8
OWN = 64
ALL = OWN + EDGE
DUMMY = ALL
CHUNK = 4
CHUNKS = ALL // CHUNK
FWD_PARTS = 1
BWD_PARTS = 2


def dot(a, b, ca, cb):
    return lax.dot_general(a, b, (((ca,), (cb,)), ((), ())), preferred_element_type=F32)


def split3(a):
    high = a.astype(BF16).astype(F32)
    rest = a - high
    mid = rest.astype(BF16).astype(F32)
    return high, mid, rest - mid


def factor_rows(left, right):
    lh, lm, ll = split3(left)
    rh, rm, rl = split3(right)
    return (
        jnp.concatenate([lh, lh, lm, lm, lh, ll], axis=1),
        jnp.concatenate([rh, rm, rh, rm, rl, rh], axis=1),
        rh,
        rm,
    )


def rows_of(shape):
    return lax.broadcasted_iota(jnp.int32, shape, 1)


def exponent_rows(x, row):
    coupling = jnp.log2(jnp.where(row == 6, x, 1.0))
    n = jnp.sum(
        jnp.where(row < 3, (-0.5 * LOG2E) * x * x, coupling), axis=1, keepdims=True
    )
    left = jnp.where(row < 3, LOG2E * x, jnp.where(row == 3, n, jnp.where(row == 4, 1.0, 0.0)))
    right = jnp.where(row < 3, x, jnp.where(row == 3, 1.0, jnp.where(row == 4, n, 0.0)))
    return left, right


def put_exponents(x, first, le, re):
    count = x.shape[0]
    left, right = exponent_rows(x, rows_of(x.shape))
    lrows, rrows, high, mid = factor_rows(left, right)
    le[pl.ds(first, count)] = lrows
    re[pl.ds(first, count)] = rrows.astype(BF16)
    return high, mid


def put_slopes(x, c, first, ld, rd, fx):
    count = x.shape[0]
    row = rows_of(x.shape)
    x3 = pltpu.roll(x, 3, 1)
    c3 = pltpu.roll(c, 3, 1)
    s = jnp.sum(jnp.where(row < 3, x * c, 0.0), axis=1, keepdims=True)
    left = jnp.where(
        row < 3, c, jnp.where(row < 6, x3, jnp.where(row == 6, s, 1.0))
    )
    right = jnp.where(
        row < 3, -x, jnp.where(row < 6, -c3, jnp.where(row == 6, 1.0, s))
    )
    lrows, rrows, high, mid = factor_rows(left, right)
    ld[pl.ds(first, count)] = lrows
    rd[pl.ds(first, count)] = rrows.astype(BF16)
    fx[pl.ds(first, count)] = jnp.concatenate([high, mid], axis=1).astype(BF16)
    return high + mid


def put_dummy(le, re, fx, more=()):
    row = lax.broadcasted_iota(jnp.int32, (48, LANES), 0)
    le[DUMMY] = jnp.zeros((48, LANES), F32)
    re[DUMMY] = jnp.where((row == 4) | (row == 20), FAR, 0.0).astype(BF16)
    fx[DUMMY] = jnp.zeros((16, LANES), BF16)
    for ref, dtype in more:
        ref[DUMMY] = jnp.zeros((48, LANES), dtype)


def pair_sums(qs, le, re, fx, outs, weights, parts, slopes=None):
    def stage(chunk, bufs):
        for u in range(CHUNK):
            p = chunk * CHUNK + u
            q1 = qs[2 * p]
            q2 = qs[2 * p + 1]
            left = jnp.transpose(le[p]).astype(BF16)
            right = jnp.concatenate([re[q1], re[q2]], axis=1)
            w = jnp.exp2(dot(left, right, 1, 0))
            values = [w]
            if slopes is not None:
                ld, rd = slopes
                left = jnp.transpose(ld[p]).astype(BF16)
                right = jnp.concatenate([rd[q1], rd[q2]], axis=1)
                values.append(w * dot(left, right, 1, 0))
            for buf, value in zip(bufs, values):
                high = value.astype(BF16)
                buf[u, 0] = high
                if parts == 2:
                    buf[u, 1] = (value - high.astype(F32)).astype(BF16)

    def drain(chunk, bufs):
        found = []
        for u in range(CHUNK):
            p = chunk * CHUNK + u
            q1 = qs[2 * p]
            q2 = qs[2 * p + 1]
            fp = fx[p]
            fq = jnp.concatenate([fx[q1], fx[q2]], axis=1)
            for out, buf in zip(outs, bufs):
                to_p = 0.0
                to_q = 0.0
                for k in range(parts):
                    w = buf[u, k]
                    to_q = to_q + dot(fp, w, 1, 0)
                    to_p = to_p + dot(fq, w, 1, 1)
                found.append((out, p, q1, q2, to_p[:8] + to_p[8:], to_q[:8] + to_q[8:]))
        for out, p, q1, q2, to_p, to_q in found:
            out[p] += to_p
            out[q1] += to_q[:, :LANES]
            out[q2] += to_q[:, LANES:]

    even, odd = weights
    stage(0, even)

    def step(i, carry):
        drain(2 * i, even)
        stage(2 * i + 1, odd)
        drain(2 * i + 1, odd)
        stage(2 * i + 2, even)
        return carry

    lax.fori_loop(0, CHUNKS // 2 - 1, step, 0)
    drain(CHUNKS - 2, even)
    stage(CHUNKS - 1, odd)
    drain(CHUNKS - 1, odd)


def row_total(block, r):
    row = lax.broadcasted_iota(jnp.int32, block.shape, 0)
    return jnp.sum(jnp.where(row == r, block, 0.0), keepdims=True)


def block_sum(a):
    return jnp.sum(a, axis=0)


def thermostat(total_k, target, atoms_all):
    state = 2.0 * total_k / (3 * atoms_all) + KINETIC_EPSILON
    return state, jnp.sqrt(1.0 + THERMO_RELAX * (target / state - 1.0))


def put_message(msg, state, sums, edge):
    msg[0:EDGE] = state[pl.ds(edge, EDGE)]
    row = lax.broadcasted_iota(jnp.int32, (8, LANES), 0)
    block = jnp.zeros((8, LANES), F32)
    for r, value in enumerate(sums):
        total = jnp.sum(value, axis=0, keepdims=True)
        block = block + jnp.where(row == r, total, 0.0)
    msg[EDGE] = block


def forward_kernel(n, steps, atoms_all):
    half_step = 0.5 * TIME_STEP
    last = n == steps

    def body(*refs):
        refs = list(refs)
        qs, par, temps = refs[:3]
        del refs[:3]
        xu, got = refs[:2]
        del refs[:2]
        if n > 0:
            g, sent = refs[:2]
            del refs[:2]
        if last:
            adj, self_sum = refs[:2]
            del refs[:2]
        xu_out, g_out, xh_out, msg = refs[:4]
        del refs[:4]
        if n > 1:
            scal = refs.pop(0)
        le, re, fx, acc, tmp, w0, w1 = refs
        edge = par[0]
        row = rows_of((OWN, 8, LANES))
        state = xu[...]
        halo = got[0:EDGE]
        velocity = pltpu.roll(state, 5, 1)
        if n > 0:
            pull = g[...]
            if n == 1:
                factor = jnp.ones((1, 1), F32)
            else:
                both = sent[EDGE] + got[EDGE]
                target = temps[0] if n - 2 < steps // 2 else temps[1]
                present, factor = thermostat(row_total(both, 0), target, atoms_all)
                r8 = lax.broadcasted_iota(jnp.int32, (8, LANES), 0)
                scal[...] = jnp.where(
                    r8 == 0, jnp.broadcast_to(factor, (8, LANES)), jnp.broadcast_to(present, (8, LANES))
                )
                if n - 1 == steps // 2:
                    factor = factor * temps[2]
            factor = factor.reshape(1, 1, 1)
            mid = factor * velocity + pull
            state = jnp.where(row < 3, state + TIME_STEP * mid, state)
            hrow = rows_of((EDGE, 8, LANES))
            halo = jnp.where(
                hrow < 3, halo + (TIME_STEP * factor) * pltpu.roll(halo, 5, 1), halo
            )
        else:
            mid = velocity
        tmp[...] = mid
        xu_out[...] = state
        xh_out[...] = halo
        high, low = put_exponents(state, 0, le, re)
        fx[pl.ds(0, OWN)] = jnp.concatenate([high, low], axis=1).astype(BF16)
        high, low = put_exponents(halo, OWN, le, re)
        fx[pl.ds(OWN, EDGE)] = jnp.concatenate([high, low], axis=1).astype(BF16)
        put_dummy(le, re, fx)
        acc[...] = jnp.zeros_like(acc)
        pair_sums(qs, le, re, fx, (acc,), ((w0,), (w1,)), FWD_PARTS)
        state = xu_out[...]
        xhat = state.astype(BF16).astype(F32)
        xhat = xhat + (state - xhat).astype(BF16).astype(F32)
        sums = acc[pl.ds(0, OWN)]
        total = sums[:, 3:4, :]
        force = 0.25 * (xhat * total - sums)
        inv_mass = state[:, 7:8, :]
        pull = half_step * inv_mass * force
        if n == 0:
            updated = tmp[...]
        else:
            updated = tmp[...] + pull
        g_out[...] = pull
        shown = pltpu.roll(updated, 3, 1)
        state = jnp.where((row >= 3) & (row < 6), shown, state)
        xu_out[...] = state
        three = row < 3
        kinetic = block_sum(jnp.where(three, 0.5 * updated * updated / inv_mass, 0.0))
        partial = [kinetic]
        if last:
            cot = adj[...]
            cot_v = pltpu.roll(cot, 5, 1)
            partial.append(block_sum(jnp.where(row == 3, 0.125 * sums, 0.0)) - self_sum[...])
            partial.append(block_sum(jnp.where(three, cot_v * updated, 0.0)))
            tmp[...] = jnp.where(three, half_step * inv_mass * cot_v, state)
        else:
            tmp[...] = jnp.where(three, state + TIME_STEP * pull, state)
        put_message(msg, tmp, partial, edge)

    return body


def backward_kernel(n, steps, atoms_all):
    half_step = 0.5 * TIME_STEP
    first = n == steps
    swap_at = steps // 2

    def body(*refs):
        refs = list(refs)
        qs, par, temps, xu, xh, av, got, sent = refs[:8]
        del refs[:8]
        uh = None
        if 0 < n < steps:
            uh, scal = refs[:2]
            del refs[:2]
        if n > 1:
            prev = refs.pop(0)
        av_out = refs.pop(0)
        if n > 0:
            msg = refs.pop(0)
        if first:
            fv_out, pass_out = refs[:2]
            del refs[:2]
        elif n == 0:
            pass
        le, re, fx, ld, rd, acc_w, acc_v, tmp, w0, w1, v0, v1 = refs
        edge = par[0]
        row = rows_of((OWN, 8, LANES))
        hrow = rows_of((EDGE, 8, LANES))
        state = xu[...]
        inv_mass = state[:, 7:8, :]
        cot = av[...]
        cot_v = pltpu.roll(cot, 5, 1)
        halo = xh[...]
        pushed = half_step * inv_mass * cot_v
        moved = got[0:EDGE]
        if n > 0:
            both = sent[EDGE] + got[EDGE]
            target = temps[0] if n - 1 < swap_at else temps[1]
            if first:
                present, factor = thermostat(row_total(both, 0), target, atoms_all)
                partner_u = moved
            else:
                factor = scal[0:1, 0:1]
                present = scal[1:2, 0:1]
                partner_u = uh[0:EDGE]
            inner = row_total(both, 2)
            slope = (
                (-THERMO_RELAX)
                * target
                / (present * present)
                * (2.0 / (3 * atoms_all))
                / (2.0 * factor)
            )
            kappa = (inner * slope).reshape(1, 1, 1)
            factor = factor.reshape(1, 1, 1)
            updated = pltpu.roll(state, 5, 1)
            if first:
                weight = factor
                r8 = lax.broadcasted_iota(jnp.int32, (8, LANES), 0)
                energy = jnp.broadcast_to(row_total(both, 1) / atoms_all, (8, LANES))
                pass_out[...] = energy
                fv_out[...] = jnp.where(row < 3, state, pltpu.roll(factor * updated, 3, 1))
            elif n - 1 == swap_at - 1:
                weight = factor + temps[3]
            else:
                weight = factor + 1.0
            cot_updated = factor * cot_v + kappa * updated / inv_mass
            tmp[...] = cot_updated
            own_c = weight * pushed + (half_step * kappa) * updated
            halo_c = weight * moved + (half_step * kappa) * pltpu.roll(partner_u, 5, 1)
        else:
            own_c = pushed
            halo_c = moved
        put_exponents(state, 0, le, re)
        put_exponents(halo, OWN, le, re)
        put_slopes(state, own_c, 0, ld, rd, fx)
        put_slopes(halo, halo_c, OWN, ld, rd, fx)
        put_dummy(le, re, fx, ((ld, F32), (rd, BF16)))
        acc_w[...] = jnp.zeros_like(acc_w)
        acc_v[...] = jnp.zeros_like(acc_v)
        pair_sums(
            qs, le, re, fx, (acc_w, acc_v), ((w0, v0), (w1, v1)), BWD_PARTS, slopes=(ld, rd)
        )
        mine = fx[pl.ds(0, OWN)].astype(F32)
        mine = mine[:, :8] + mine[:, 8:]
        sums_w = acc_w[pl.ds(0, OWN)]
        sums_v = acc_v[pl.ds(0, OWN)]
        total_w = sums_w[:, 6:7, :]
        total_v = sums_v[:, 6:7, :]
        from_w = pltpu.roll(sums_w - mine * total_w, 5, 1)
        from_v = sums_v - mine * total_v
        gradient = 0.25 * (from_w - from_v)
        state = xu[...]
        cot = av[...]
        inv_mass = state[:, 7:8, :]
        three = row < 3
        cot = jnp.where(three, cot + gradient, cot)
        coupling = 0.25 * total_v / state[:, 6:7, :]
        cot = jnp.where(row == 6, cot + coupling, cot)
        if n == 0:
            av_out[...] = cot
        else:
            cot_mid = tmp[...] + TIME_STEP * cot
            if n - 1 == swap_at:
                cot_mid = cot_mid * temps[2]
            if first:
                cot = jnp.where(row == 7, pass_out[0:1, 0:1].reshape(1, 1, 1), cot)
            cot = jnp.where((row >= 3) & (row < 6), pltpu.roll(cot_mid, 3, 1), cot)
            av_out[...] = cot
            tmp[...] = jnp.where(three, half_step * inv_mass * cot_mid, 0.0)
            zero = jnp.zeros((8, LANES), F32)
            partial = [zero, zero]
            if n > 1:
                before = pltpu.roll(prev[...], 5, 1)
                partial.append(block_sum(jnp.where(three, cot_mid * before, 0.0)))
            put_message(msg, tmp, partial, edge)

    return body


def shape(*dims):
    return jax.ShapeDtypeStruct(dims, F32)


def vmem():
    return pl.BlockSpec(memory_space=pltpu.VMEM)


def smem():
    return pl.BlockSpec(memory_space=pltpu.SMEM)


def scratch_of(backward):
    blocks = DUMMY + 1
    parts = BWD_PARTS if backward else FWD_PARTS
    weight = pltpu.VMEM((CHUNK, parts, LANES, 2 * LANES), BF16)
    acc = pltpu.VMEM((blocks, 8, LANES), F32)
    left = pltpu.VMEM((blocks, 48, LANES), F32)
    right = pltpu.VMEM((blocks, 48, LANES), BF16)
    found = [left, right, pltpu.VMEM((blocks, 16, LANES), BF16)]
    if backward:
        found += [left, right, acc]
    found += [acc, pltpu.VMEM((OWN, 8, LANES), F32), weight, weight]
    if backward:
        found += [weight, weight]
    return found


def run_kernel(body, name, ints, arrays, out_shapes, backward):
    return pl.pallas_call(
        body,
        in_specs=[smem() for _ in ints] + [vmem() for _ in arrays],
        out_specs=[vmem() for _ in out_shapes],
        out_shape=out_shapes,
        scratch_shapes=scratch_of(backward),
        name=name,
    )(*ints, *arrays)


def quarter_spot(i):
    return (0, 2, 1, 3)[i]


def local(
    starting_locations,
    starting_speeds,
    terminal_location_adjoint,
    terminal_speed_adjoint,
    interaction_strength,
    reciprocal_particle_weight,
    heat_levels,
    swap_indicator,
    companion_group_indices,
):
    count = lax.axis_size("atom")
    atoms_all = starting_locations.shape[2] * count
    steps = companion_group_indices.shape[0] - 1
    spot = lax.axis_index("atom")
    lane_of_four = spot % 4
    core = spot % 2
    replica = spot // 4

    partner = lax.ppermute(heat_levels, "rep", [(i, i ^ 1) for i in range(lax.axis_size("rep"))])
    later = jnp.where(swap_indicator == 1, partner, heat_levels)
    mine = jnp.arange(4) == replica
    t1 = jnp.sum(jnp.where(mine, heat_levels, 0.0))
    t2 = jnp.sum(jnp.where(mine, later, 0.0))
    temps = jnp.stack([t1, t2, jnp.sqrt(t2 / t1), jnp.sqrt(t1 / t2)])

    def blocks(a):
        return a.reshape(a.shape[0], a.shape[1], EDGE, LANES).transpose(0, 2, 1, 3)

    shared = jnp.stack([interaction_strength, reciprocal_particle_weight])
    shared = jnp.broadcast_to(shared[None], (4, *shared.shape))
    start = blocks(jnp.concatenate([starting_locations, starting_speeds, shared], axis=1))
    adjoint = blocks(
        jnp.concatenate(
            [terminal_location_adjoint, terminal_speed_adjoint, jnp.zeros_like(shared)], axis=1
        )
    )
    lists = companion_group_indices.astype(F32).reshape(1, 1, 1, -1)
    lists = jnp.pad(lists, ((0, 0), (0, 0), (0, 7), (0, LANES - lists.shape[3])))
    lists = jnp.broadcast_to(lists, (4, 1, 8, LANES))
    outgoing = jnp.concatenate([start, lists, adjoint], axis=1)
    quarter = []
    for s in range(4):
        sent = lax.dynamic_index_in_dim(outgoing, (lane_of_four + s) % 4, 0, False)
        quarter.append(
            lax.ppermute(
                sent,
                "atom",
                [(i, 4 * ((i % 4 + s) % 4) + quarter_spot(i // 4)) for i in range(count)],
            )
        )
    order = jnp.concatenate([q[None] for q in reversed(quarter)] * 2, axis=0)
    quarter = lax.dynamic_slice_in_dim(order, (3 - replica) % 4, 4, 0)
    swap = [(i, i ^ 2) for i in range(count)]
    bit = (spot // 2) % 2

    def both_quarters(a):
        other = lax.ppermute(a, "atom", swap)
        low = jnp.where(bit == 0, a, other)
        high = jnp.where(bit == 0, other, a)
        return jnp.concatenate([low, high], axis=0)

    early = both_quarters(quarter[:, : EDGE + 1])
    late = both_quarters(quarter[:, EDGE + 1 :])
    xu = early[:, :EDGE].reshape(OWN, 8, LANES)
    adj = late.reshape(OWN, 8, LANES)
    pair = [(i, i ^ 1) for i in range(count)]

    def exchange(a):
        return lax.ppermute(a, "atom", pair)

    beside = jnp.where(core == 0, early[-1], early[0])
    got = exchange(beside)
    edge = jnp.where(core == 0, OWN - EDGE, 0).astype(jnp.int32).reshape(1)

    def listed(a):
        return a[..., EDGE, 0, : 10 * EDGE].astype(jnp.int32)

    slots = listed(early).reshape(8, 5, EDGE, 2).transpose(1, 0, 2, 3)
    shard = 8 * core + jnp.arange(8, dtype=jnp.int32)
    block = (shard * EDGE - EDGE)[None, :, None, None] + slots
    block = block.reshape(5, OWN, 2)
    here = block - OWN * core
    halo_first = jnp.where(core == 0, OWN, OWN - EDGE)
    beyond = block - halo_first
    own_q = jnp.where(
        (here >= 0) & (here < OWN),
        here,
        jnp.where((beyond >= 0) & (beyond < EDGE), OWN + beyond, DUMMY),
    )
    halo_shard = jnp.where(core == 0, 8, 7)
    halo_q = listed(got).reshape(5, EDGE, 2) + (halo_shard * EDGE - EDGE) - OWN * core
    halo_q = jnp.where((halo_q >= 0) & (halo_q < OWN), halo_q, DUMMY)
    pairs = jnp.concatenate([own_q, halo_q], axis=1).reshape(5, 2 * ALL)
    selves = jnp.any(own_q[steps] == jnp.arange(OWN, dtype=jnp.int32)[:, None], axis=1)
    self_sum = jnp.sum(
        jnp.where(selves[:, None], 0.25 * xu[:, 6, :] * xu[:, 6, :], 0.0), axis=0, keepdims=True
    )
    self_sum = jnp.pad(self_sum, ((0, 7), (0, 0)))

    full = shape(OWN, 8, LANES)
    part = shape(EDGE, 8, LANES)
    message = shape(EDGE + 1, 8, LANES)
    scalars = shape(8, LANES)

    states, halos, received, sents, scal = [], [], [got], [None], {}
    g = None
    for n in range(steps + 1):
        arrays = [xu, received[n]]
        if n > 0:
            arrays += [g, sents[n]]
        if n == steps:
            arrays += [adj, self_sum]
        outs = [full, full, part, message]
        if n > 1:
            outs.append(scalars)
        found = run_kernel(
            forward_kernel(n, steps, atoms_all),
            f"force_{n}",
            [pairs[n], edge, temps],
            arrays,
            outs,
            False,
        )
        xu, g, xh, msg = found[:4]
        if n > 1:
            scal[n - 1] = found[4]
        states.append(xu)
        halos.append(xh)
        sents.append(msg)
        received.append(exchange(msg))

    av = adj
    got, sent = received[steps + 1], sents[steps + 1]
    for n in reversed(range(steps + 1)):
        arrays = [states[n], halos[n], av, got, sent]
        if 0 < n < steps:
            arrays += [received[n + 1], scal[n]]
        if n > 1:
            arrays.append(states[n - 1])
        outs = [full]
        if n > 0:
            outs.append(message)
        if n == steps:
            outs += [full, scalars]
        found = run_kernel(
            backward_kernel(n, steps, atoms_all),
            f"adjoint_{n}",
            [pairs[n], edge, temps],
            arrays,
            outs,
            True,
        )
        av = found[0]
        if n == steps:
            final = found[2]
        if n > 0:
            sent = found[1]
            got = exchange(sent)

    results = jnp.concatenate([final, av], axis=1).reshape(8, EDGE, 16, LANES)
    returned = []
    for s in range(4):
        kk = (replica - s) % 4
        piece = lax.dynamic_index_in_dim(results, 4 * bit + kk, 0, False)
        returned.append(
            lax.ppermute(
                piece,
                "atom",
                [(4 * ((i % 4 + s) % 4) + quarter_spot(i // 4), i) for i in range(count)],
            )
        )
    order = jnp.concatenate([r[None] for r in returned] * 2, axis=0)
    back = lax.dynamic_slice_in_dim(order, (4 - lane_of_four) % 4, 4, 0)

    def rows(first, size):
        a = back[:, :, first : first + size].transpose(0, 2, 1, 3)
        return a.reshape(4, size, EDGE * LANES)

    energies = back[:, 0, 15, 0]
    coupling = jnp.sum(back[:, :, 14], axis=0).reshape(-1)
    copies = jnp.broadcast_to(coupling, (lax.axis_size("rep"), *coupling.shape))
    everything = lax.all_to_all(copies, "rep", split_axis=0, concat_axis=0, tiled=True)
    grad_coupling = jnp.sum(everything, axis=0)
    return (rows(0, 3), rows(3, 3), energies, rows(8, 3), rows(11, 3), grad_coupling)


def solution(mesh):
    in_specs = (
        P("rep", None, "atom"),
        P("rep", None, "atom"),
        P("rep", None, "atom"),
        P("rep", None, "atom"),
        P("atom"),
        P("atom"),
        P("rep"),
        P("rep"),
        P(None, "atom", None),
    )
    out_specs = (
        P("rep", None, "atom"),
        P("rep", None, "atom"),
        P("rep"),
        P("rep", None, "atom"),
        P("rep", None, "atom"),
        P("atom"),
    )
    return jax.shard_map(local, mesh=mesh, in_specs=in_specs, out_specs=out_specs, check_vma=False)
```

```python
import jax
import jax.numpy as jnp
from jax import lax
from jax.experimental import pallas as pl
from jax.experimental.pallas import tpu as pltpu
from jax.sharding import PartitionSpec as P

TIME_STEP = 0.05
THERMO_RELAX = 0.5
KINETIC_EPSILON = 1e-06
LOG2E = 1.4426950408889634
FAR = -1.0e5

F32 = jnp.float32
BF16 = jnp.bfloat16

LANES = 128
EDGE = 8
OWN = 64
ALL = OWN + EDGE
DUMMY = ALL
CHUNK = 4
CHUNKS = ALL // CHUNK
ROOM = ALL + CHUNK
LISTED = 2 * ROOM
GROUP = 8
FWD_PARTS = 1
BWD_PARTS = 2


def dot(a, b, ca, cb):
    return lax.dot_general(a, b, (((ca,), (cb,)), ((), ())), preferred_element_type=F32)


def split3(a):
    high = a.astype(BF16).astype(F32)
    rest = a - high
    mid = rest.astype(BF16).astype(F32)
    return high, mid, rest - mid


def factor_rows(left, right):
    lh, lm, ll = split3(left)
    rh, rm, rl = split3(right)
    return (
        jnp.concatenate([lh, lh, lm, lm, lh, ll], axis=1),
        jnp.concatenate([rh, rm, rh, rm, rl, rh], axis=1),
        rh,
        rm,
    )


def rows_of(shape):
    return lax.broadcasted_iota(jnp.int32, shape, 1)


def exponent_rows(x, row):
    coupling = jnp.log2(jnp.where(row == 6, x, 1.0))
    n = jnp.sum(
        jnp.where(row < 3, (-0.5 * LOG2E) * x * x, coupling), axis=1, keepdims=True
    )
    left = jnp.where(row < 3, LOG2E * x, jnp.where(row == 3, n, jnp.where(row == 4, 1.0, 0.0)))
    right = jnp.where(row < 3, x, jnp.where(row == 3, 1.0, jnp.where(row == 4, n, 0.0)))
    return left, right


def put_exponents(x, row, at, le, re, fx=None):
    left, right = exponent_rows(x, row)
    lrows, rrows, high, mid = factor_rows(left, right)
    le[at] = lrows
    re[at] = rrows.astype(BF16)
    if fx is not None:
        fx[at] = jnp.concatenate([high, mid], axis=1).astype(BF16)


def put_slopes(x, c, row, at, ld, rd, fx):
    x3 = pltpu.roll(x, 3, 1)
    c3 = pltpu.roll(c, 3, 1)
    s = jnp.sum(jnp.where(row < 3, x * c, 0.0), axis=1, keepdims=True)
    left = jnp.where(row < 3, c, jnp.where(row < 6, x3, jnp.where(row == 6, s, 1.0)))
    right = jnp.where(row < 3, -x, jnp.where(row < 6, -c3, jnp.where(row == 6, 1.0, s)))
    lrows, rrows, high, mid = factor_rows(left, right)
    ld[at] = lrows
    rd[at] = rrows.astype(BF16)
    fx[at] = jnp.concatenate([high, mid], axis=1).astype(BF16)


def put_dummy(le, re, fx, more=()):
    row = lax.broadcasted_iota(jnp.int32, (48, LANES), 0)
    le[DUMMY] = jnp.zeros((48, LANES), F32)
    re[DUMMY] = jnp.where((row == 4) | (row == 20), FAR, 0.0).astype(BF16)
    fx[DUMMY] = jnp.zeros((16, LANES), BF16)
    for ref, dtype in more:
        ref[DUMMY] = jnp.zeros((48, LANES), dtype)


def pair_sums(qs, base, le, re, fx, outs, weights, parts, slopes=None):
    def stage(chunk, bufs):
        for u in range(CHUNK):
            p = chunk * CHUNK + u
            q1 = qs[base + 2 * p]
            q2 = qs[base + 2 * p + 1]
            left = jnp.transpose(le[p]).astype(BF16)
            right = jnp.concatenate([re[q1], re[q2]], axis=1)
            w = jnp.exp2(dot(left, right, 1, 0))
            values = [w]
            if slopes is not None:
                ld, rd = slopes
                left = jnp.transpose(ld[p]).astype(BF16)
                right = jnp.concatenate([rd[q1], rd[q2]], axis=1)
                values.append(w * dot(left, right, 1, 0))
            for buf, value in zip(bufs, values):
                high = value.astype(BF16)
                buf[u, 0] = high
                if parts == 2:
                    buf[u, 1] = (value - high.astype(F32)).astype(BF16)

    def drain(chunk, bufs):
        found = []
        for u in range(CHUNK):
            p = chunk * CHUNK + u
            q1 = qs[base + 2 * p]
            q2 = qs[base + 2 * p + 1]
            fp = fx[p]
            fq = jnp.concatenate([fx[q1], fx[q2]], axis=1)
            for out, buf in zip(outs, bufs):
                to_p = 0.0
                to_q = 0.0
                for k in range(parts):
                    w = buf[u, k]
                    to_q = to_q + dot(fp, w, 1, 0)
                    to_p = to_p + dot(fq, w, 1, 1)
                found.append((out, p, q1, q2, to_p[:8] + to_p[8:], to_q[:8] + to_q[8:]))
        for out, p, q1, q2, to_p, to_q in found:
            out[p] += to_p
            out[q1] += to_q[:, :LANES]
            out[q2] += to_q[:, LANES:]

    even, odd = weights
    stage(0, even)

    def step(i, carry):
        drain(2 * i, even)
        stage(2 * i + 1, odd)
        drain(2 * i + 1, odd)
        stage(2 * i + 2, even)
        return carry

    lax.fori_loop(0, CHUNKS // 2, step, 0)


def row_total(block, r):
    row = lax.broadcasted_iota(jnp.int32, block.shape, 0)
    return jnp.sum(jnp.where(row == r, block, 0.0), keepdims=True)


def block_sum(a):
    return jnp.sum(a, axis=0)


def thermostat(total_k, target, atoms_all):
    state = 2.0 * total_k / (3 * atoms_all) + KINETIC_EPSILON
    return state, jnp.sqrt(1.0 + THERMO_RELAX * (target / state - 1.0))


def put_message(msg, state, sums, edge):
    msg[0:EDGE] = state[pl.ds(edge, EDGE)]
    row = lax.broadcasted_iota(jnp.int32, (8, LANES), 0)
    block = jnp.zeros((8, LANES), F32)
    for r, value in enumerate(sums):
        if value is not None:
            total = jnp.sum(value, axis=0, keepdims=True)
            block = block + jnp.where(row == r, total, 0.0)
    msg[EDGE] = block


def group_rows():
    return rows_of((GROUP, 8, LANES))


def over_groups(body, init=0):
    return lax.fori_loop(0, OWN // GROUP, lambda i, c: body(pl.ds(i * GROUP, GROUP), c), init)


def clear(*accs):
    def body(at, carry):
        for acc in accs:
            acc[at] = jnp.zeros((GROUP, 8, LANES), F32)
        return carry

    over_groups(body)
    for acc in accs:
        acc[pl.ds(OWN, EDGE)] = jnp.zeros((EDGE, 8, LANES), F32)
        acc[DUMMY] = jnp.zeros((8, LANES), F32)


def forward_kernel(n, steps, atoms_all):
    half_step = 0.5 * TIME_STEP
    last = n == steps
    base = n * LISTED
    zero = (8, LANES)

    def body(*refs):
        refs = list(refs)
        ints, temps, xu, got = refs[:4]
        del refs[:4]
        if n > 0:
            g, sent = refs[:2]
            del refs[:2]
        if last:
            adj, self_sum = refs[:2]
            del refs[:2]
        xu_out, g_out, xh_out, msg = refs[:4]
        del refs[:4]
        if n > 1:
            scal = refs.pop(0)
        le, re, fx, acc, tmp, w0, w1 = refs
        edge = ints[(steps + 1) * LISTED]
        if n > 0:
            factor = jnp.ones((1, 1), F32)
            if n > 1:
                both = sent[EDGE] + got[EDGE]
                target = temps[0] if n - 2 < steps // 2 else temps[1]
                present, factor = thermostat(row_total(both, 0), target, atoms_all)
                r8 = lax.broadcasted_iota(jnp.int32, zero, 0)
                scal[...] = jnp.where(
                    r8 == 0, jnp.broadcast_to(factor, zero), jnp.broadcast_to(present, zero)
                )
                if n - 1 == steps // 2:
                    factor = factor * temps[2]
            factor = factor.reshape(1, 1, 1)

        def prepare(at, carry):
            row = group_rows()
            state = xu[at]
            mid = pltpu.roll(state, 5, 1)
            if n > 0:
                mid = factor * mid + g[at]
                state = jnp.where(row < 3, state + TIME_STEP * mid, state)
            tmp[at] = mid
            xu_out[at] = state
            put_exponents(state, row, at, le, re, fx)
            return carry

        over_groups(prepare)
        row = rows_of((EDGE, 8, LANES))
        halo = got[0:EDGE]
        if n > 0:
            halo = jnp.where(row < 3, halo + (TIME_STEP * factor) * pltpu.roll(halo, 5, 1), halo)
        xh_out[...] = halo
        put_exponents(halo, row, pl.ds(OWN, EDGE), le, re, fx)
        put_dummy(le, re, fx)
        clear(acc)
        pair_sums(ints, base, le, re, fx, (acc,), ((w0,), (w1,)), FWD_PARTS)

        def finish(at, carry):
            row = group_rows()
            three = row < 3
            state = xu_out[at]
            high = state.astype(BF16).astype(F32)
            sums = acc[at]
            total = sums[:, 3:4, :]
            force = 0.25 * ((high + (state - high).astype(BF16).astype(F32)) * total - sums)
            inv_mass = state[:, 7:8, :]
            pull = half_step * inv_mass * force
            updated = tmp[at]
            if n > 0:
                updated = updated + pull
            g_out[at] = pull
            state = jnp.where((row >= 3) & (row < 6), pltpu.roll(updated, 3, 1), state)
            xu_out[at] = state
            found = [block_sum(jnp.where(three, 0.5 * updated * updated / inv_mass, 0.0))]
            if last:
                cot_v = pltpu.roll(adj[at], 5, 1)
                found.append(block_sum(jnp.where(row == 3, 0.125 * sums, 0.0)))
                found.append(block_sum(jnp.where(three, cot_v * updated, 0.0)))
                tmp[at] = jnp.where(three, half_step * inv_mass * cot_v, state)
            else:
                tmp[at] = jnp.where(three, state + TIME_STEP * pull, state)
            return tuple(c + f for c, f in zip(carry, found))

        partial = list(over_groups(finish, (jnp.zeros(zero, F32),) * (3 if last else 1)))
        if last:
            partial[1] = partial[1] - self_sum[...]
        put_message(msg, tmp, partial, edge)

    return body


def backward_kernel(n, steps, atoms_all):
    half_step = 0.5 * TIME_STEP
    first = n == steps
    swap_at = steps // 2
    base = n * LISTED
    zero = (8, LANES)

    def body(*refs):
        refs = list(refs)
        ints, temps, xu, xh, av, got = refs[:6]
        del refs[:6]
        if n > 0:
            sent = refs.pop(0)
        if 0 < n < steps:
            uh, scal = refs[:2]
            del refs[:2]
        if n > 1:
            before = refs.pop(0)
        if n == 0:
            final = refs.pop(0)
        av_out = refs.pop(0)
        if n > 0:
            msg = refs.pop(0)
        if first:
            fv_out = refs.pop(0)
        le, re, fx, ld, rd, acc_w, acc_v, tmp, w0, w1, v0, v1 = refs
        edge = ints[(steps + 1) * LISTED]
        if n > 0:
            both = sent[EDGE] + got[EDGE]
            target = temps[0] if n - 1 < swap_at else temps[1]
            if first:
                present, factor = thermostat(row_total(both, 0), target, atoms_all)
                energy = (row_total(both, 1) / atoms_all).reshape(1, 1, 1)
            else:
                factor = scal[0:1, 0:1]
                present = scal[1:2, 0:1]
            inner = row_total(both, 2)
            slope = (
                (-THERMO_RELAX)
                * target
                / (present * present)
                * (2.0 / (3 * atoms_all))
                / (2.0 * factor)
            )
            kappa = (inner * slope).reshape(1, 1, 1)
            factor = factor.reshape(1, 1, 1)
            if first:
                weight = factor
            elif n == swap_at:
                weight = factor + temps[3]
            else:
                weight = factor + 1.0

        def prepare(at, carry):
            row = group_rows()
            state = xu[at]
            inv_mass = state[:, 7:8, :]
            cot_v = pltpu.roll(av[at], 5, 1)
            own_c = half_step * inv_mass * cot_v
            if n > 0:
                updated = pltpu.roll(state, 5, 1)
                tmp[at] = factor * cot_v + kappa * updated / inv_mass
                own_c = weight * own_c + (half_step * kappa) * updated
                if first:
                    fv_out[at] = jnp.where(row < 3, state, factor * state)
            put_exponents(state, row, at, le, re)
            put_slopes(state, own_c, row, at, ld, rd, fx)
            return carry

        over_groups(prepare)
        row = rows_of((EDGE, 8, LANES))
        halo = xh[...]
        halo_c = got[0:EDGE]
        if n > 0:
            partner_u = halo_c if first else uh[0:EDGE]
            halo_c = weight * halo_c + (half_step * kappa) * pltpu.roll(partner_u, 5, 1)
        put_exponents(halo, row, pl.ds(OWN, EDGE), le, re)
        put_slopes(halo, halo_c, row, pl.ds(OWN, EDGE), ld, rd, fx)
        put_dummy(le, re, fx, ((ld, F32), (rd, BF16)))
        clear(acc_w, acc_v)
        pair_sums(
            ints,
            base,
            le,
            re,
            fx,
            (acc_w, acc_v),
            ((w0, v0), (w1, v1)),
            BWD_PARTS,
            slopes=(ld, rd),
        )

        def finish(at, carry):
            row = group_rows()
            three = row < 3
            own = fx[at].astype(F32)
            own = own[:, :8] + own[:, 8:]
            sums_w = acc_w[at]
            sums_v = acc_v[at]
            total_v = sums_v[:, 6:7, :]
            from_w = pltpu.roll(sums_w - own * sums_w[:, 6:7, :], 5, 1)
            gradient = 0.25 * (from_w - (sums_v - own * total_v))
            state = xu[at]
            inv_mass = state[:, 7:8, :]
            cot = av[at]
            cot = jnp.where(three, cot + gradient, cot)
            cot = jnp.where(row == 6, cot + 0.25 * total_v / state[:, 6:7, :], cot)
            if n == 0:
                av_out[at] = jnp.concatenate([final[at], cot], axis=1)
                return carry
            cot_mid = tmp[at] + TIME_STEP * cot
            if n - 1 == swap_at:
                cot_mid = cot_mid * temps[2]
            if first:
                cot = jnp.where(row == 7, energy, cot)
            cot = jnp.where((row >= 3) & (row < 6), pltpu.roll(cot_mid, 3, 1), cot)
            av_out[at] = cot
            tmp[at] = jnp.where(three, half_step * inv_mass * cot_mid, 0.0)
            if n > 1:
                held = pltpu.roll(before[at], 5, 1)
                carry = carry + block_sum(jnp.where(three, cot_mid * held, 0.0))
            return carry

        inner = over_groups(finish, jnp.zeros(zero, F32))
        if n > 0:
            put_message(msg, tmp, [None, None, inner if n > 1 else None], edge)

    return body


def shape(*dims):
    return pltpu.VMEM(dims, F32)


def vmem():
    return pl.BlockSpec(memory_space=pltpu.VMEM)


def smem():
    return pl.BlockSpec(memory_space=pltpu.SMEM)


def scratch_of(backward):
    blocks = ROOM
    parts = BWD_PARTS if backward else FWD_PARTS
    weight = pltpu.VMEM((CHUNK, parts, LANES, 2 * LANES), BF16)
    acc = pltpu.VMEM((blocks, 8, LANES), F32)
    left = pltpu.VMEM((blocks, 48, LANES), F32)
    right = pltpu.VMEM((blocks, 48, LANES), BF16)
    found = [left, right, pltpu.VMEM((blocks, 16, LANES), BF16)]
    if backward:
        found += [left, right, acc]
    found += [acc, pltpu.VMEM((OWN, 8, LANES), F32), weight, weight]
    if backward:
        found += [weight, weight]
    return found


def run_kernel(body, name, ints, temps, arrays, out_shapes, backward):
    arrays = [pltpu.with_memory_space_constraint(a, pltpu.VMEM) for a in arrays]
    return pl.pallas_call(
        body,
        in_specs=[smem(), smem()] + [vmem() for _ in arrays],
        out_specs=[vmem() for _ in out_shapes],
        out_shape=out_shapes,
        scratch_shapes=scratch_of(backward),
        name=name,
    )(ints, temps, *arrays)


def quarter_spot(i):
    return (0, 2, 1, 3)[i]


def local(
    starting_locations,
    starting_speeds,
    terminal_location_adjoint,
    terminal_speed_adjoint,
    interaction_strength,
    reciprocal_particle_weight,
    heat_levels,
    swap_indicator,
    companion_group_indices,
):
    count = lax.axis_size("atom")
    atoms_all = starting_locations.shape[2] * count
    steps = companion_group_indices.shape[0] - 1
    spot = lax.axis_index("atom")
    lane_of_four = spot % 4
    core = spot % 2
    replica = spot // 4

    partner = lax.ppermute(heat_levels, "rep", [(i, i ^ 1) for i in range(lax.axis_size("rep"))])
    later = jnp.where(swap_indicator == 1, partner, heat_levels)
    mine = jnp.arange(4) == replica
    t1 = jnp.sum(jnp.where(mine, heat_levels, 0.0))
    t2 = jnp.sum(jnp.where(mine, later, 0.0))
    temps = jnp.stack([t1, t2, jnp.sqrt(t2 / t1), jnp.sqrt(t1 / t2)])

    def blocks(a):
        return a.reshape(a.shape[0], a.shape[1], EDGE, LANES).transpose(0, 2, 1, 3)

    shared = jnp.stack([interaction_strength, reciprocal_particle_weight])
    shared = jnp.broadcast_to(shared[None], (4, *shared.shape))
    start = blocks(jnp.concatenate([starting_locations, starting_speeds, shared], axis=1))
    adjoint = blocks(
        jnp.concatenate(
            [terminal_location_adjoint, terminal_speed_adjoint, jnp.zeros_like(shared)], axis=1
        )
    )
    lists = companion_group_indices.astype(F32).reshape(1, 1, 1, -1)
    lists = jnp.pad(lists, ((0, 0), (0, 0), (0, 7), (0, LANES - lists.shape[3])))
    lists = jnp.broadcast_to(lists, (4, 1, 8, LANES))
    outgoing = jnp.concatenate([start, lists, adjoint], axis=1)
    quarter = []
    for s in range(4):
        sent = lax.dynamic_index_in_dim(outgoing, (lane_of_four + s) % 4, 0, False)
        quarter.append(
            lax.ppermute(
                sent,
                "atom",
                [(i, 4 * ((i % 4 + s) % 4) + quarter_spot(i // 4)) for i in range(count)],
            )
        )
    order = jnp.concatenate([q[None] for q in reversed(quarter)] * 2, axis=0)
    quarter = lax.dynamic_slice_in_dim(order, (3 - replica) % 4, 4, 0)
    swap = [(i, i ^ 2) for i in range(count)]
    bit = (spot // 2) % 2

    def both_quarters(a):
        other = lax.ppermute(a, "atom", swap)
        low = jnp.where(bit == 0, a, other)
        high = jnp.where(bit == 0, other, a)
        return jnp.concatenate([low, high], axis=0)

    early = both_quarters(quarter[:, : EDGE + 1])
    late = both_quarters(quarter[:, EDGE + 1 :])
    xu = early[:, :EDGE].reshape(OWN, 8, LANES)
    adj = late.reshape(OWN, 8, LANES)
    pair = [(i, i ^ 1) for i in range(count)]

    def exchange(a):
        return lax.ppermute(a, "atom", pair)

    beside = jnp.where(core == 0, early[-1], early[0])
    got = exchange(beside)
    edge = jnp.where(core == 0, OWN - EDGE, 0).astype(jnp.int32)

    def listed(a):
        return a[..., EDGE, 0, : 10 * EDGE].astype(jnp.int32)

    slots = listed(early).reshape(8, 5, EDGE, 2).transpose(1, 0, 2, 3)
    shard = 8 * core + jnp.arange(8, dtype=jnp.int32)
    block = (shard * EDGE - EDGE)[None, :, None, None] + slots
    block = block.reshape(5, OWN, 2)
    here = block - OWN * core
    halo_first = jnp.where(core == 0, OWN, OWN - EDGE)
    beyond = block - halo_first
    own_q = jnp.where(
        (here >= 0) & (here < OWN),
        here,
        jnp.where((beyond >= 0) & (beyond < EDGE), OWN + beyond, DUMMY),
    )
    halo_shard = jnp.where(core == 0, 8, 7)
    halo_q = listed(got).reshape(5, EDGE, 2) + (halo_shard * EDGE - EDGE) - OWN * core
    halo_q = jnp.where((halo_q >= 0) & (halo_q < OWN), halo_q, DUMMY)
    pairs = jnp.concatenate([own_q, halo_q], axis=1)
    pairs = jnp.pad(pairs, ((0, 0), (0, ROOM - ALL), (0, 0)), constant_values=DUMMY)
    ints = jnp.concatenate([pairs.reshape(-1), jnp.broadcast_to(edge, (8,))])
    selves = jnp.any(own_q[steps] == jnp.arange(OWN, dtype=jnp.int32)[:, None], axis=1)
    self_sum = jnp.sum(
        jnp.where(selves[:, None], 0.25 * xu[:, 6, :] * xu[:, 6, :], 0.0), axis=0, keepdims=True
    )
    self_sum = jnp.pad(self_sum, ((0, 7), (0, 0)))

    full = shape(OWN, 8, LANES)
    part = shape(EDGE, 8, LANES)
    message = shape(EDGE + 1, 8, LANES)
    scalars = shape(8, LANES)

    states, halos, received, sents, scal = [], [], [got], [None], {}
    g = None
    for n in range(steps + 1):
        arrays = [xu, received[n]]
        if n > 0:
            arrays += [g, sents[n]]
        if n == steps:
            arrays += [adj, self_sum]
        outs = [full, full, part, message]
        if n > 1:
            outs.append(scalars)
        found = run_kernel(
            forward_kernel(n, steps, atoms_all),
            f"force_{n}",
            ints,
            temps,
            arrays,
            outs,
            False,
        )
        xu, g, xh, msg = found[:4]
        if n > 1:
            scal[n - 1] = found[4]
        states.append(xu)
        halos.append(xh)
        sents.append(msg)
        received.append(exchange(msg))

    av = adj
    got, sent = received[steps + 1], sents[steps + 1]
    for n in reversed(range(steps + 1)):
        arrays = [states[n], halos[n], av, got]
        if n > 0:
            arrays.append(sent)
        if 0 < n < steps:
            arrays += [received[n + 1], scal[n]]
        if n > 1:
            arrays.append(states[n - 1])
        if n == 0:
            arrays.append(final)
        outs = [full, message] if n > 0 else [shape(OWN, 16, LANES)]
        if n == steps:
            outs.append(full)
        found = run_kernel(
            backward_kernel(n, steps, atoms_all), f"adjoint_{n}", ints, temps, arrays, outs, True
        )
        av = found[0]
        if n == steps:
            final = found[2]
        if n > 0:
            sent = found[1]
            got = exchange(sent)

    results = av.reshape(8, EDGE, 16, LANES)
    returned = []
    for s in range(4):
        kk = (replica - s) % 4
        piece = lax.dynamic_index_in_dim(results, 4 * bit + kk, 0, False)
        returned.append(
            lax.ppermute(
                piece,
                "atom",
                [(4 * ((i % 4 + s) % 4) + quarter_spot(i // 4), i) for i in range(count)],
            )
        )
    order = jnp.concatenate([r[None] for r in returned] * 2, axis=0)
    back = lax.dynamic_slice_in_dim(order, (4 - lane_of_four) % 4, 4, 0)

    def rows(first, size):
        a = back[:, :, first : first + size].transpose(0, 2, 1, 3)
        return a.reshape(4, size, EDGE * LANES)

    energies = back[:, 0, 15, 0]
    coupling = jnp.sum(back[:, :, 14], axis=0).reshape(-1)
    copies = jnp.broadcast_to(coupling, (lax.axis_size("rep"), *coupling.shape))
    everything = lax.all_to_all(copies, "rep", split_axis=0, concat_axis=0, tiled=True)
    grad_coupling = jnp.sum(everything, axis=0)
    return (rows(0, 3), rows(3, 3), energies, rows(8, 3), rows(11, 3), grad_coupling)


def solution(mesh):
    in_specs = (
        P("rep", None, "atom"),
        P("rep", None, "atom"),
        P("rep", None, "atom"),
        P("rep", None, "atom"),
        P("atom"),
        P("atom"),
        P("rep"),
        P("rep"),
        P(None, "atom", None),
    )
    out_specs = (
        P("rep", None, "atom"),
        P("rep", None, "atom"),
        P("rep"),
        P("rep", None, "atom"),
        P("rep", None, "atom"),
        P("atom"),
    )
    return jax.shard_map(local, mesh=mesh, in_specs=in_specs, out_specs=out_specs, check_vma=False)
```

```python
import jax
import jax.numpy as jnp
from jax import lax
from jax.experimental import pallas as pl
from jax.experimental.pallas import tpu as pltpu
from jax.sharding import PartitionSpec as P

TIME_STEP = 0.05
THERMO_RELAX = 0.5
KINETIC_EPSILON = 1e-06
LOG2E = 1.4426950408889634
FAR = -1.0e5

F32 = jnp.float32
BF16 = jnp.bfloat16

LANES = 128
EDGE = 8
OWN = 64
ALL = OWN + EDGE
DUMMY = ALL
FWD_CHUNK = 9
BWD_CHUNK = 4
ROOM = ALL + max(FWD_CHUNK, BWD_CHUNK)
LISTED = 2 * ROOM
GROUP = 8
FWD_PARTS = 1
BWD_PARTS = 2


def dot(a, b, ca, cb):
    return lax.dot_general(a, b, (((ca,), (cb,)), ((), ())), preferred_element_type=F32)


def split3(a):
    high = a.astype(BF16).astype(F32)
    rest = a - high
    mid = rest.astype(BF16).astype(F32)
    return high, mid, rest - mid


def factor_rows(left, right):
    lh, lm, ll = split3(left)
    rh, rm, rl = split3(right)
    return (
        jnp.concatenate([lh, lh, lm, lm, lh, ll], axis=1),
        jnp.concatenate([rh, rm, rh, rm, rl, rh], axis=1),
        rh,
        rm,
    )


def rows_of(shape):
    return lax.broadcasted_iota(jnp.int32, shape, 1)


def exponent_rows(x, row):
    coupling = jnp.log2(jnp.where(row == 6, x, 1.0))
    n = jnp.sum(
        jnp.where(row < 3, (-0.5 * LOG2E) * x * x, coupling), axis=1, keepdims=True
    )
    left = jnp.where(row < 3, LOG2E * x, jnp.where(row == 3, n, jnp.where(row == 4, 1.0, 0.0)))
    right = jnp.where(row < 3, x, jnp.where(row == 3, 1.0, jnp.where(row == 4, n, 0.0)))
    return left, right


def put_exponents(x, row, at, le, re, fx=None):
    left, right = exponent_rows(x, row)
    lrows, rrows, high, mid = factor_rows(left, right)
    le[at] = lrows
    re[at] = rrows.astype(BF16)
    if fx is not None:
        fx[at] = jnp.concatenate([high, mid], axis=1).astype(BF16)


def put_slopes(x, c, row, at, ld, rd, fx):
    x3 = pltpu.roll(x, 3, 1)
    c3 = pltpu.roll(c, 3, 1)
    s = jnp.sum(jnp.where(row < 3, x * c, 0.0), axis=1, keepdims=True)
    left = jnp.where(row < 3, c, jnp.where(row < 6, x3, jnp.where(row == 6, s, 1.0)))
    right = jnp.where(row < 3, -x, jnp.where(row < 6, -c3, jnp.where(row == 6, 1.0, s)))
    lrows, rrows, high, mid = factor_rows(left, right)
    ld[at] = lrows
    rd[at] = rrows.astype(BF16)
    fx[at] = jnp.concatenate([high, mid], axis=1).astype(BF16)


def put_dummy(le, re, fx, more=()):
    row = lax.broadcasted_iota(jnp.int32, (48, LANES), 0)
    le[DUMMY] = jnp.zeros((48, LANES), F32)
    re[DUMMY] = jnp.where((row == 4) | (row == 20), FAR, 0.0).astype(BF16)
    fx[DUMMY] = jnp.zeros((16, LANES), BF16)
    for ref, dtype in more:
        ref[DUMMY] = jnp.zeros((48, LANES), dtype)


def pair_sums(qs, base, le, re, fx, outs, weights, parts, chunk, slopes=None):
    def stage_one(index, u, bufs):
        p = index * chunk + u
        q1 = qs[base + 2 * p]
        q2 = qs[base + 2 * p + 1]
        left = jnp.transpose(le[p]).astype(BF16)
        right = jnp.concatenate([re[q1], re[q2]], axis=1)
        w = jnp.exp2(dot(left, right, 1, 0))
        values = [w]
        if slopes is not None:
            ld, rd = slopes
            left = jnp.transpose(ld[p]).astype(BF16)
            right = jnp.concatenate([rd[q1], rd[q2]], axis=1)
            values.append(w * dot(left, right, 1, 0))
        for buf, value in zip(bufs, values):
            high = value.astype(BF16)
            buf[u, 0] = high
            if parts == 2:
                buf[u, 1] = (value - high.astype(F32)).astype(BF16)

    def drain_one(index, u, bufs):
        found = []
        p = index * chunk + u
        q1 = qs[base + 2 * p]
        q2 = qs[base + 2 * p + 1]
        fp = fx[p]
        fq = jnp.concatenate([fx[q1], fx[q2]], axis=1)
        for out, buf in zip(outs, bufs):
            to_p = 0.0
            to_q = 0.0
            for k in range(parts):
                w = buf[u, k]
                to_q = to_q + dot(fp, w, 1, 0)
                to_p = to_p + dot(fq, w, 1, 1)
            found.append((out, p, q1, q2, to_p[:8] + to_p[8:], to_q[:8] + to_q[8:]))
        return found

    def add(found):
        for out, p, q1, q2, to_p, to_q in found:
            out[p] += to_p
            out[q1] += to_q[:, :LANES]
            out[q2] += to_q[:, LANES:]

    even, odd = weights

    def both(full_chunk, full, next_chunk, empty):
        waiting = []
        for u in range(chunk):
            stage_one(next_chunk, u, empty)
            waiting += drain_one(full_chunk, u, full)
        add(waiting)

    for u in range(chunk):
        stage_one(0, u, even)

    def step(i, carry):
        both(2 * i, even, 2 * i + 1, odd)
        both(2 * i + 1, odd, 2 * i + 2, even)
        return carry

    lax.fori_loop(0, ALL // (2 * chunk), step, 0)


def row_total(block, r):
    row = lax.broadcasted_iota(jnp.int32, block.shape, 0)
    return jnp.sum(jnp.where(row == r, block, 0.0), keepdims=True)


def block_sum(a):
    return jnp.sum(a, axis=0)


def thermostat(total_k, target, atoms_all):
    state = 2.0 * total_k / (3 * atoms_all) + KINETIC_EPSILON
    return state, jnp.sqrt(1.0 + THERMO_RELAX * (target / state - 1.0))


def put_message(msg, state, sums, edge):
    msg[0:EDGE] = state[pl.ds(edge, EDGE)]
    row = lax.broadcasted_iota(jnp.int32, (8, LANES), 0)
    block = jnp.zeros((8, LANES), F32)
    for r, value in enumerate(sums):
        if value is not None:
            total = jnp.sum(value, axis=0, keepdims=True)
            block = block + jnp.where(row == r, total, 0.0)
    msg[EDGE] = block


def group_rows():
    return rows_of((GROUP, 8, LANES))


def over_groups(body, init=0):
    return lax.fori_loop(0, OWN // GROUP, lambda i, c: body(pl.ds(i * GROUP, GROUP), c), init)


def clear(*accs):
    def body(at, carry):
        for acc in accs:
            acc[at] = jnp.zeros((GROUP, 8, LANES), F32)
        return carry

    over_groups(body)
    for acc in accs:
        acc[pl.ds(OWN, EDGE)] = jnp.zeros((EDGE, 8, LANES), F32)
        acc[DUMMY] = jnp.zeros((8, LANES), F32)


def forward_kernel(n, steps, atoms_all):
    half_step = 0.5 * TIME_STEP
    last = n == steps
    base = n * LISTED
    zero = (8, LANES)

    def body(*refs):
        refs = list(refs)
        ints, temps, xu, got = refs[:4]
        del refs[:4]
        if n > 0:
            g, sent = refs[:2]
            del refs[:2]
        if last:
            adj, self_sum = refs[:2]
            del refs[:2]
        xu_out, g_out, xh_out, msg = refs[:4]
        del refs[:4]
        if n > 1:
            scal = refs.pop(0)
        le, re, fx, acc, tmp, w0, w1 = refs
        edge = ints[(steps + 1) * LISTED]
        if n > 0:
            factor = jnp.ones((1, 1), F32)
            if n > 1:
                both = sent[EDGE] + got[EDGE]
                target = temps[0] if n - 2 < steps // 2 else temps[1]
                present, factor = thermostat(row_total(both, 0), target, atoms_all)
                r8 = lax.broadcasted_iota(jnp.int32, zero, 0)
                scal[...] = jnp.where(
                    r8 == 0, jnp.broadcast_to(factor, zero), jnp.broadcast_to(present, zero)
                )
                if n - 1 == steps // 2:
                    factor = factor * temps[2]
            factor = factor.reshape(1, 1, 1)

        def prepare(at, carry):
            row = group_rows()
            state = xu[at]
            mid = pltpu.roll(state, 5, 1)
            if n > 0:
                mid = factor * mid + g[at]
                state = jnp.where(row < 3, state + TIME_STEP * mid, state)
            tmp[at] = mid
            xu_out[at] = state
            put_exponents(state, row, at, le, re, fx)
            return carry

        over_groups(prepare)
        row = rows_of((EDGE, 8, LANES))
        halo = got[0:EDGE]
        if n > 0:
            halo = jnp.where(row < 3, halo + (TIME_STEP * factor) * pltpu.roll(halo, 5, 1), halo)
        xh_out[...] = halo
        put_exponents(halo, row, pl.ds(OWN, EDGE), le, re, fx)
        put_dummy(le, re, fx)
        clear(acc)
        pair_sums(ints, base, le, re, fx, (acc,), ((w0,), (w1,)), FWD_PARTS, FWD_CHUNK)

        def finish(at, carry):
            row = group_rows()
            three = row < 3
            state = xu_out[at]
            high = state.astype(BF16).astype(F32)
            sums = acc[at]
            total = sums[:, 3:4, :]
            force = 0.25 * ((high + (state - high).astype(BF16).astype(F32)) * total - sums)
            inv_mass = state[:, 7:8, :]
            pull = half_step * inv_mass * force
            updated = tmp[at]
            if n > 0:
                updated = updated + pull
            g_out[at] = pull
            state = jnp.where((row >= 3) & (row < 6), pltpu.roll(updated, 3, 1), state)
            xu_out[at] = state
            found = [block_sum(jnp.where(three, 0.5 * updated * updated / inv_mass, 0.0))]
            if last:
                cot_v = pltpu.roll(adj[at], 5, 1)
                found.append(block_sum(jnp.where(row == 3, 0.125 * sums, 0.0)))
                found.append(block_sum(jnp.where(three, cot_v * updated, 0.0)))
                tmp[at] = jnp.where(three, half_step * inv_mass * cot_v, state)
            else:
                tmp[at] = jnp.where(three, state + TIME_STEP * pull, state)
            return tuple(c + f for c, f in zip(carry, found))

        partial = list(over_groups(finish, (jnp.zeros(zero, F32),) * (3 if last else 1)))
        if last:
            partial[1] = partial[1] - self_sum[...]
        put_message(msg, tmp, partial, edge)

    return body


def backward_kernel(n, steps, atoms_all):
    half_step = 0.5 * TIME_STEP
    first = n == steps
    swap_at = steps // 2
    base = n * LISTED
    zero = (8, LANES)

    def body(*refs):
        refs = list(refs)
        ints, temps, xu, xh, av, got = refs[:6]
        del refs[:6]
        if n > 0:
            sent = refs.pop(0)
        if 0 < n < steps:
            uh, scal = refs[:2]
            del refs[:2]
        if n > 1:
            before = refs.pop(0)
        if n == 0:
            final = refs.pop(0)
        av_out = refs.pop(0)
        if n > 0:
            msg = refs.pop(0)
        if first:
            fv_out = refs.pop(0)
        le, re, fx, ld, rd, acc_w, acc_v, tmp, w0, w1, v0, v1 = refs
        edge = ints[(steps + 1) * LISTED]
        if n > 0:
            both = sent[EDGE] + got[EDGE]
            target = temps[0] if n - 1 < swap_at else temps[1]
            if first:
                present, factor = thermostat(row_total(both, 0), target, atoms_all)
                energy = (row_total(both, 1) / atoms_all).reshape(1, 1, 1)
            else:
                factor = scal[0:1, 0:1]
                present = scal[1:2, 0:1]
            inner = row_total(both, 2)
            slope = (
                (-THERMO_RELAX)
                * target
                / (present * present)
                * (2.0 / (3 * atoms_all))
                / (2.0 * factor)
            )
            kappa = (inner * slope).reshape(1, 1, 1)
            factor = factor.reshape(1, 1, 1)
            if first:
                weight = factor
            elif n == swap_at:
                weight = factor + temps[3]
            else:
                weight = factor + 1.0

        def prepare(at, carry):
            row = group_rows()
            state = xu[at]
            inv_mass = state[:, 7:8, :]
            cot_v = pltpu.roll(av[at], 5, 1)
            own_c = half_step * inv_mass * cot_v
            if n > 0:
                updated = pltpu.roll(state, 5, 1)
                tmp[at] = factor * cot_v + kappa * updated / inv_mass
                own_c = weight * own_c + (half_step * kappa) * updated
                if first:
                    fv_out[at] = jnp.where(row < 3, state, factor * state)
            put_exponents(state, row, at, le, re)
            put_slopes(state, own_c, row, at, ld, rd, fx)
            return carry

        over_groups(prepare)
        row = rows_of((EDGE, 8, LANES))
        halo = xh[...]
        halo_c = got[0:EDGE]
        if n > 0:
            partner_u = halo_c if first else uh[0:EDGE]
            halo_c = weight * halo_c + (half_step * kappa) * pltpu.roll(partner_u, 5, 1)
        put_exponents(halo, row, pl.ds(OWN, EDGE), le, re)
        put_slopes(halo, halo_c, row, pl.ds(OWN, EDGE), ld, rd, fx)
        put_dummy(le, re, fx, ((ld, F32), (rd, BF16)))
        clear(acc_w, acc_v)
        pair_sums(
            ints,
            base,
            le,
            re,
            fx,
            (acc_w, acc_v),
            ((w0, v0), (w1, v1)),
            BWD_PARTS,
            BWD_CHUNK,
            slopes=(ld, rd),
        )

        def finish(at, carry):
            row = group_rows()
            three = row < 3
            own = fx[at].astype(F32)
            own = own[:, :8] + own[:, 8:]
            sums_w = acc_w[at]
            sums_v = acc_v[at]
            total_v = sums_v[:, 6:7, :]
            from_w = pltpu.roll(sums_w - own * sums_w[:, 6:7, :], 5, 1)
            gradient = 0.25 * (from_w - (sums_v - own * total_v))
            state = xu[at]
            inv_mass = state[:, 7:8, :]
            cot = av[at]
            cot = jnp.where(three, cot + gradient, cot)
            cot = jnp.where(row == 6, cot + 0.25 * total_v / state[:, 6:7, :], cot)
            if n == 0:
                av_out[at] = jnp.concatenate([final[at], cot], axis=1)
                return carry
            cot_mid = tmp[at] + TIME_STEP * cot
            if n - 1 == swap_at:
                cot_mid = cot_mid * temps[2]
            if first:
                cot = jnp.where(row == 7, energy, cot)
            cot = jnp.where((row >= 3) & (row < 6), pltpu.roll(cot_mid, 3, 1), cot)
            av_out[at] = cot
            tmp[at] = jnp.where(three, half_step * inv_mass * cot_mid, 0.0)
            if n > 1:
                held = pltpu.roll(before[at], 5, 1)
                carry = carry + block_sum(jnp.where(three, cot_mid * held, 0.0))
            return carry

        inner = over_groups(finish, jnp.zeros(zero, F32))
        if n > 0:
            put_message(msg, tmp, [None, None, inner if n > 1 else None], edge)

    return body


def shape(*dims):
    return pltpu.VMEM(dims, F32)


def vmem():
    return pl.BlockSpec(memory_space=pltpu.VMEM)


def smem():
    return pl.BlockSpec(memory_space=pltpu.SMEM)


def scratch_of(backward):
    blocks = ROOM
    parts = BWD_PARTS if backward else FWD_PARTS
    chunk = BWD_CHUNK if backward else FWD_CHUNK
    weight = pltpu.VMEM((chunk, parts, LANES, 2 * LANES), BF16)
    acc = pltpu.VMEM((blocks, 8, LANES), F32)
    left = pltpu.VMEM((blocks, 48, LANES), F32)
    right = pltpu.VMEM((blocks, 48, LANES), BF16)
    found = [left, right, pltpu.VMEM((blocks, 16, LANES), BF16)]
    if backward:
        found += [left, right, acc]
    found += [acc, pltpu.VMEM((OWN, 8, LANES), F32), weight, weight]
    if backward:
        found += [weight, weight]
    return found


def run_kernel(body, name, ints, temps, arrays, out_shapes, backward):
    arrays = [pltpu.with_memory_space_constraint(a, pltpu.VMEM) for a in arrays]
    return pl.pallas_call(
        body,
        in_specs=[smem(), smem()] + [vmem() for _ in arrays],
        out_specs=[vmem() for _ in out_shapes],
        out_shape=out_shapes,
        scratch_shapes=scratch_of(backward),
        name=name,
    )(ints, temps, *arrays)


def quarter_spot(i):
    return (0, 2, 1, 3)[i]


def local(
    starting_locations,
    starting_speeds,
    terminal_location_adjoint,
    terminal_speed_adjoint,
    interaction_strength,
    reciprocal_particle_weight,
    heat_levels,
    swap_indicator,
    companion_group_indices,
):
    count = lax.axis_size("atom")
    atoms_all = starting_locations.shape[2] * count
    steps = companion_group_indices.shape[0] - 1
    spot = lax.axis_index("atom")
    lane_of_four = spot % 4
    core = spot % 2
    replica = spot // 4

    partner = lax.ppermute(heat_levels, "rep", [(i, i ^ 1) for i in range(lax.axis_size("rep"))])
    later = jnp.where(swap_indicator == 1, partner, heat_levels)
    mine = jnp.arange(4) == replica
    t1 = jnp.sum(jnp.where(mine, heat_levels, 0.0))
    t2 = jnp.sum(jnp.where(mine, later, 0.0))
    temps = jnp.stack([t1, t2, jnp.sqrt(t2 / t1), jnp.sqrt(t1 / t2)])

    def blocks(a):
        return a.reshape(a.shape[0], a.shape[1], EDGE, LANES).transpose(0, 2, 1, 3)

    shared = jnp.stack([interaction_strength, reciprocal_particle_weight])
    shared = jnp.broadcast_to(shared[None], (4, *shared.shape))
    start = blocks(jnp.concatenate([starting_locations, starting_speeds, shared], axis=1))
    adjoint = blocks(
        jnp.concatenate(
            [terminal_location_adjoint, terminal_speed_adjoint, jnp.zeros_like(shared)], axis=1
        )
    )
    lists = companion_group_indices.astype(F32).reshape(1, 1, 1, -1)
    lists = jnp.pad(lists, ((0, 0), (0, 0), (0, 7), (0, LANES - lists.shape[3])))
    lists = jnp.broadcast_to(lists, (4, 1, 8, LANES))
    outgoing = jnp.concatenate([start, lists, adjoint], axis=1)
    quarter = []
    for s in range(4):
        sent = lax.dynamic_index_in_dim(outgoing, (lane_of_four + s) % 4, 0, False)
        quarter.append(
            lax.ppermute(
                sent,
                "atom",
                [(i, 4 * ((i % 4 + s) % 4) + quarter_spot(i // 4)) for i in range(count)],
            )
        )
    order = jnp.concatenate([q[None] for q in reversed(quarter)] * 2, axis=0)
    quarter = lax.dynamic_slice_in_dim(order, (3 - replica) % 4, 4, 0)
    swap = [(i, i ^ 2) for i in range(count)]
    bit = (spot // 2) % 2

    def both_quarters(a):
        other = lax.ppermute(a, "atom", swap)
        low = jnp.where(bit == 0, a, other)
        high = jnp.where(bit == 0, other, a)
        return jnp.concatenate([low, high], axis=0)

    early = both_quarters(quarter[:, : EDGE + 1])
    xu = early[:, :EDGE].reshape(OWN, 8, LANES)
    pair = [(i, i ^ 1) for i in range(count)]

    def exchange(a):
        return lax.ppermute(a, "atom", pair)

    beside = jnp.where(core == 0, early[-1], early[0])
    got = exchange(beside)
    edge = jnp.where(core == 0, OWN - EDGE, 0).astype(jnp.int32)

    def listed(a):
        return a[..., EDGE, 0, : 10 * EDGE].astype(jnp.int32)

    slots = listed(early).reshape(8, 5, EDGE, 2).transpose(1, 0, 2, 3)
    shard = 8 * core + jnp.arange(8, dtype=jnp.int32)
    block = (shard * EDGE - EDGE)[None, :, None, None] + slots
    block = block.reshape(5, OWN, 2)
    here = block - OWN * core
    halo_first = jnp.where(core == 0, OWN, OWN - EDGE)
    beyond = block - halo_first
    own_q = jnp.where(
        (here >= 0) & (here < OWN),
        here,
        jnp.where((beyond >= 0) & (beyond < EDGE), OWN + beyond, DUMMY),
    )
    halo_shard = jnp.where(core == 0, 8, 7)
    halo_q = listed(got).reshape(5, EDGE, 2) + (halo_shard * EDGE - EDGE) - OWN * core
    halo_q = jnp.where((halo_q >= 0) & (halo_q < OWN), halo_q, DUMMY)
    pairs = jnp.concatenate([own_q, halo_q], axis=1)
    pairs = jnp.pad(pairs, ((0, 0), (0, ROOM - ALL), (0, 0)), constant_values=DUMMY)
    ints = jnp.concatenate([pairs.reshape(-1), jnp.broadcast_to(edge, (8,))])
    selves = jnp.any(own_q[steps] == jnp.arange(OWN, dtype=jnp.int32)[:, None], axis=1)
    self_sum = jnp.sum(
        jnp.where(selves[:, None], 0.25 * xu[:, 6, :] * xu[:, 6, :], 0.0), axis=0, keepdims=True
    )
    self_sum = jnp.pad(self_sum, ((0, 7), (0, 0)))

    full = shape(OWN, 8, LANES)
    part = shape(EDGE, 8, LANES)
    message = shape(EDGE + 1, 8, LANES)
    scalars = shape(8, LANES)

    states, halos, received, sents, scal = [], [], [got], [None], {}
    g = None
    for n in range(steps + 1):
        arrays = [xu, received[n]]
        if n > 0:
            arrays += [g, sents[n]]
        if n == steps:
            arrays += [adj, self_sum]
        outs = [full, full, part, message]
        if n > 1:
            outs.append(scalars)
        found = run_kernel(
            forward_kernel(n, steps, atoms_all),
            f"force_{n}",
            ints,
            temps,
            arrays,
            outs,
            False,
        )
        xu, g, xh, msg = found[:4]
        if n > 1:
            scal[n - 1] = found[4]
        states.append(xu)
        halos.append(xh)
        sents.append(msg)
        received.append(exchange(msg))
        if n == 0:
            late, _ = lax.optimization_barrier((quarter[:, EDGE + 1 :], received[1]))
            adj = both_quarters(late).reshape(OWN, 8, LANES)

    av = adj
    got, sent = received[steps + 1], sents[steps + 1]
    for n in reversed(range(steps + 1)):
        arrays = [states[n], halos[n], av, got]
        if n > 0:
            arrays.append(sent)
        if 0 < n < steps:
            arrays += [received[n + 1], scal[n]]
        if n > 1:
            arrays.append(states[n - 1])
        if n == 0:
            arrays.append(final)
        outs = [full, message] if n > 0 else [shape(OWN, 16, LANES)]
        if n == steps:
            outs.append(full)
        found = run_kernel(
            backward_kernel(n, steps, atoms_all), f"adjoint_{n}", ints, temps, arrays, outs, True
        )
        av = found[0]
        if n == steps:
            final = found[2]
        if n > 0:
            sent = found[1]
            got = exchange(sent)

    results = av.reshape(8, EDGE, 16, LANES)
    returned = []
    for s in range(4):
        kk = (replica - s) % 4
        piece = lax.dynamic_index_in_dim(results, 4 * bit + kk, 0, False)
        returned.append(
            lax.ppermute(
                piece,
                "atom",
                [(4 * ((i % 4 + s) % 4) + quarter_spot(i // 4), i) for i in range(count)],
            )
        )
    order = jnp.concatenate([r[None] for r in returned] * 2, axis=0)
    back = lax.dynamic_slice_in_dim(order, (4 - lane_of_four) % 4, 4, 0)

    def rows(first, size):
        a = back[:, :, first : first + size].transpose(0, 2, 1, 3)
        return a.reshape(4, size, EDGE * LANES)

    energies = back[:, 0, 15, 0]
    coupling = jnp.sum(back[:, :, 14], axis=0).reshape(-1)
    copies = jnp.broadcast_to(coupling, (lax.axis_size("rep"), *coupling.shape))
    everything = lax.all_to_all(copies, "rep", split_axis=0, concat_axis=0, tiled=True)
    grad_coupling = jnp.sum(everything, axis=0)
    return (rows(0, 3), rows(3, 3), energies, rows(8, 3), rows(11, 3), grad_coupling)


def solution(mesh):
    in_specs = (
        P("rep", None, "atom"),
        P("rep", None, "atom"),
        P("rep", None, "atom"),
        P("rep", None, "atom"),
        P("atom"),
        P("atom"),
        P("rep"),
        P("rep"),
        P(None, "atom", None),
    )
    out_specs = (
        P("rep", None, "atom"),
        P("rep", None, "atom"),
        P("rep"),
        P("rep", None, "atom"),
        P("rep", None, "atom"),
        P("atom"),
    )
    return jax.shard_map(local, mesh=mesh, in_specs=in_specs, out_specs=out_specs, check_vma=False)
```
